256 devices in a mesh: seq: 64 (over z, y, core), rep: 4 (over x).
Axes of the slice: x: 4, y: 4, z: 8, core: 2. Of those that a mesh axis runs over, the one named last changes fastest.
Arguments:
- inputs: bfloat16 [4, 8192, 1024], P('rep', 'seq'), may hold values from -6 to 6
- weight_t: bfloat16 [3072, 1024], P('seq', 'rep'), may hold values from -0.1875 to 0.1875
- states: float32 [4, 8192, 1024], P('rep', 'seq'), may hold values from -0.9 to 0.9
- doc_ids: int32 [4, 8192], P('rep', 'seq'), may hold values from 0 to 31, never falling along the last dimension, each value on 1 to 512 neighbouring positions
- recur: float32 [3, 1024], replicated, may hold values from -1 to 1
- bias: float32 [3, 1024], replicated, may hold values from -8 to 3, as said below
- out_grad: bfloat16 [4, 8192, 1024], P('rep', 'seq'), may hold values from -6 to 6
Outputs:
- input_grad: bfloat16 [4, 8192, 1024], P('rep', 'seq')
- weight_grad: float32 [3072, 1024], P('seq', 'rep')
- param_grad: float32 [6, 1024], replicated
The draws below stay inside these ranges and needn't reach their ends.
Inputs may be any that keep to these rules, and one draw needn't show every extreme that they name: `doc_ids`: within each sequence the numbers never fall; every document has 1 to 512 tokens, and some document has exactly 512. `bias`: row 0 lies between -8 and -1, rows 1 and 2 between -3 and 3.
All inputs are finite; a program needn't handle non-finite values.
Results may differ from the reference program's by a relative error of at most 0.0095.
Values may be sent and summed in bfloat16 or wider, within the bound.
No kernel may reach another device: no remote copies, remote signals or barrier semaphores. Data moves between devices by JAX's collectives and lax.ppermute only.
A program may use at most 128 MiB of HBM per device.

```python
import math
import jax
import jax.numpy as jnp
import numpy as np
from jax import lax

DI = 1024
H = 1024
L = 8192
SEQS = 4
SEGS = 32
MOST = 512


def draw_bias(key, part):
    keys = jax.random.split(jax.random.fold_in(key, 17), 4)
    share = 0.5
    others = jnp.clip(jax.random.normal(keys[3], (2, H), jnp.float32), -3.0, 3.0)
    slower = jax.random.uniform(keys[0], (H,), jnp.float32) < share
    slow_value = jax.random.uniform(keys[1], (H,), jnp.float32, -8.0, -6.0)
    fast_value = jax.random.uniform(keys[2], (H,), jnp.float32, -3.0, -1.0)
    first = jnp.where(slower, slow_value, fast_value)
    return jnp.concatenate([first[None, :], others], 0).astype(jnp.float32)


def block_levels(rng, extent, cuts, least, high):
    level = 1.0
    for position, blocks in cuts:
        draws = jax.random.uniform(jax.random.fold_in(jax.random.fold_in(rng, 6), position), (blocks,), jnp.float32, least / len(cuts), high / len(cuts))
        level = level * jnp.repeat(jnp.exp(draws), extent[position] // blocks).reshape((-1,) + (1,) * (len(extent) - 1 - position))
    return level


def profile(amount, total, reach, slope):
    loads = [(1 << 20) // math.isqrt(standing ** slope) + 1 for standing in range(2, amount + 1)]
    spare, counts = total - reach - (amount - 1), [1] * (amount - 1)
    while spare > 0:
        candidates = [i for i in range(amount - 1) if counts[i] < reach]
        pool, budget = sum([loads[i] for i in candidates]), spare
        for i in candidates:
            addition = min(reach - counts[i], max(1, budget * loads[i] // pool), spare)
            counts[i] = counts[i] + addition
            spare = spare - addition
    return np.array([reach] + counts)


def uneven(stream_key, count, total, most, lean):
    if count == 2:
        one = jax.random.randint(stream_key, (), max(1, total - most), min(most, total - 1) + 1)
        return jnp.stack([one, total - one])
    sizes = jnp.asarray(profile(count, total, most, lean), jnp.int32)
    couples = (count - 1) // 2
    giver, receiver = sizes[1:1 + 2 * couples:2], sizes[2:2 + 2 * couples:2]
    room = jnp.minimum(giver - 1, most - receiver)
    moved = jax.random.randint(jax.random.fold_in(stream_key, 1), (couples,), 0, 1 << 20) % (room + 1)
    sizes = sizes.at[1:1 + 2 * couples:2].set(giver - moved).at[2:2 + 2 * couples:2].set(receiver + moved)
    return sizes[jax.random.permutation(jax.random.fold_in(stream_key, 2), count)]


def bell_draw(rng, extent, scale, limit, shards=(), kind=jnp.bfloat16):
    array = scale * jax.random.normal(rng, extent, jnp.float32)
    if shards:
        array = array * block_levels(rng, extent, shards, -0.22, 0.18)
    return jnp.clip(array, -limit, limit).astype(kind)


def setup_inputs(seed: int = 0) -> dict:
    key_of = jax.random.split(jax.random.key(seed), 8)
    return {
        "inputs": bell_draw(key_of[0], (SEQS, L, DI), 1.0, 6.0, ((0, 4), (1, 64))),
        "weight_t": bell_draw(key_of[1], (3 * H, DI), DI ** -0.5, 0.1875, ((0, 64), (1, 4))),
        "states": jnp.clip(jax.random.uniform(key_of[2], (SEQS, L, H), jnp.float32, -0.9, 0.9) * block_levels(key_of[2], (SEQS, L, H), ((0, 4), (1, 64)), -0.4, 0.0), -0.9, 0.9),
        "doc_ids": jax.vmap(lambda own: jnp.searchsorted(jnp.cumsum(uneven(own, SEGS, L, MOST, 1)), jnp.arange(L), side="right"))(jax.random.split(key_of[3], SEQS)).reshape((SEQS, L)).astype(jnp.int32),
        "recur": jnp.clip(jax.random.uniform(key_of[4], (3, H), jnp.float32, -1.0, 1.0), -1.0, 1.0),
        "bias": draw_bias(jax.random.fold_in(key_of[7], 71), 0),
        "out_grad": bell_draw(key_of[6], (SEQS, L, H), 1.0, 6.0, ((0, 4), (1, 64))),
    }


def one_sequence(feats, states, doc_ids, out_grad, weight_t, recur, bias):
    preact = jnp.dot(feats, weight_t.T, preferred_element_type=jnp.float32)
    pz = preact[:, :H]
    pr = preact[:, H:2 * H]
    pc = preact[:, 2 * H:]
    same = jnp.concatenate([jnp.zeros((1,), jnp.float32), (doc_ids[1:] == doc_ids[:-1]).astype(jnp.float32)])
    prior = jnp.concatenate([jnp.zeros((1, H), jnp.float32), states[:-1]], 0) * same[:, None]
    gate_z = jax.nn.sigmoid(pz + recur[0] * prior + bias[0])
    gate_r = jax.nn.sigmoid(pr + recur[1] * prior + bias[1])
    gate_c = jnp.tanh(pc + recur[2] * gate_r * prior + bias[2])
    jacobian = same[:, None] * (1.0 - gate_z + (gate_c - prior) * gate_z * (1.0 - gate_z) * recur[0] + gate_z * (1.0 - gate_c * gate_c) * recur[2] * (gate_r + prior * gate_r * (1.0 - gate_r) * recur[1]))
    factor = jnp.concatenate([jacobian[1:], jnp.zeros((1, H), jnp.float32)], 0)

    def backstep(carry, item):
        upstream, coef = item
        adjoint = upstream + coef * carry
        return (adjoint, adjoint)
    _, adjoint = lax.scan(backstep, jnp.zeros((H,), jnp.float32), (out_grad.astype(jnp.float32), factor), reverse=True)
    grad_z = adjoint * (gate_c - prior) * gate_z * (1.0 - gate_z)
    grad_c = adjoint * gate_z * (1.0 - gate_c * gate_c)
    grad_r = grad_c * recur[2] * prior * gate_r * (1.0 - gate_r)
    grad_pre = jnp.concatenate([grad_z, grad_r, grad_c], 1).astype(jnp.bfloat16)
    input_grad = jnp.dot(grad_pre, weight_t, preferred_element_type=jnp.float32).astype(jnp.bfloat16)
    weight_part = jnp.dot(grad_pre.T, feats, preferred_element_type=jnp.float32)
    stats = jnp.stack([grad_z.sum(0), grad_r.sum(0), grad_c.sum(0), (grad_z * prior).sum(0), (grad_r * prior).sum(0), (grad_c * gate_r * prior).sum(0)])
    return (input_grad, weight_part, stats)

def reference(inputs, weight_t, states, doc_ids, recur, bias, out_grad):

    def single(items):
        return one_sequence(items[0], items[1], items[2], items[3], weight_t, recur, bias)
    input_grad, weight_parts, stats = lax.map(single, (inputs, states, doc_ids, out_grad))
    factor = 1.0 / math.sqrt(SEQS * L)
    return (input_grad, weight_parts.sum(0) * factor, stats.sum(0) * factor)
```

```python
import functools
import math

import jax
import jax.numpy as jnp
from jax import lax
from jax.experimental import pallas as pl
from jax.experimental.pallas import tpu as pltpu
from jax.sharding import Mesh
from jax.sharding import PartitionSpec as P

SEQ = ("z", "y", "c")
ALL = ("z", "y", "c", "x")
NZ, NY, NC, NX = 8, 4, 2, 4
T = 128
F = 1024
H = 1024
W = 128
UNIT = 16
CB = F // 4
FAR = 2.0
CHUNK = 32
BF = jnp.bfloat16
F32 = jnp.float32


def piece_route(k):
    route = []
    for s in range(NZ * NY * NC):
        unit = 3 * s + k
        hidden = unit % 64
        share = hidden // 8
        for x in range(NX):
            z, y, c, xx = hidden % 8, x, share // 4, share % 4
            route.append((s * NX + x, ((z * NY + y) * NC + c) * NX + xx))
    return route


def around(a, axis, k):
    n = lax.axis_size(axis)
    return lax.ppermute(a, axis, [(i, (i + k) % n) for i in range(n)])


def along(a, axis, n, k):
    return lax.ppermute(a, axis, [(i, i + k) for i in range(n) if 0 <= i + k < n])


def call(body, outs, args, scratch=(), name=None):
    vmem = pl.BlockSpec(memory_space=pltpu.VMEM)
    return pl.pallas_call(
        body,
        out_shape=[jax.ShapeDtypeStruct(s, d) for s, d in outs],
        in_specs=[pl.BlockSpec(memory_space=pltpu.SMEM)] + [vmem] * (len(args) - 1),
        out_specs=[vmem] * len(outs),
        scratch_shapes=list(scratch),
        name=name,
    )(*args)


def at(start, size, step):
    return pl.ds(pl.multiple_of(start, step), size)


def split2(v):
    high = v.astype(BF)
    return high, (v - high.astype(F32)).astype(BF)


MSG = F + 3 * 2 * W


def messages_body(idx, inputs, states, ids, grads, tail, *outs):
    first = (idx[0] == 0) & (idx[1] == 0) & (idx[2] == 0)
    row = lax.broadcasted_iota(jnp.int32, (T, W), 0)
    before = jnp.where(row == 0, tail[1:2, 0:W], pltpu.roll(ids[...], 1, 0))
    same = (before == ids[...]) & ((row > 0) | jnp.logical_not(first))
    for k in range(NX):
        to = lax.rem(idx[3] + k, NX)
        outs[k][:, 0:F] = inputs[...]
        for c in range(NC):
            lanes = at(c * 512 + to * W, W, W)
            prior = jnp.where(row == 0, tail[0:1, lanes], pltpu.roll(states[:, lanes], 1, 0))
            high, low = split2(jnp.where(same, prior, FAR))
            outs[k][:, F + c * W : F + (c + 1) * W] = high
            outs[k][:, F + (2 + c) * W : F + (3 + c) * W] = low
            outs[k][:, F + (4 + c) * W : F + (5 + c) * W] = grads[:, lanes]


def forward_body(idx, recur, bias, *refs):
    blocks, refs = refs[:8], refs[8:]
    parts, refs = refs[:4], refs[4:]
    az, ac, ar, pr, rp, loc, fac, ends, weight, pre, jac, upg = refs
    z, y, c, x = idx[0], idx[1], idx[2], idx[3]
    share = c * 4 + x
    for kz in range(NZ):
        unit = lax.rem(z - kz + NZ, NZ)
        turn = lax.rem(share * 8 + unit, 3)
        for g in range(3):
            src = at(kz * 48 + lax.rem(g + turn, 3) * UNIT, UNIT, UNIT)
            dst = at(g * W + unit * UNIT, UNIT, UNIT)
            for ky in range(NY):
                weight[lax.rem(y - ky + NY, NY), dst, :] = parts[ky][src, :]
    feats = jnp.concatenate([b[:, 0:F] for k in range(4) for b in (blocks[k], blocks[4 + k])], 0)
    rows = jnp.concatenate([weight[b] for b in range(4)], 1)
    pre[...] = lax.dot_general(feats, rows, (((1,), (1,)), ((), ())), preferred_element_type=F32)
    lanes = at(share * W, W, W)
    rz, rr, rc = (recur[g : g + 1, lanes] for g in range(3))
    bz, br, bc = (bias[g : g + 1, lanes] for g in range(3))
    for k in range(4):
        jac[k, 2 * T : 2 * T + 8, :] = jnp.ones((8, W), F32)
        for side in range(2):
            block = blocks[k + 4 * side]
            base = k * 256 + side * T
            half = lax.rem(c + side, 2) * T

            def step(i, carry, block=block, base=base, half=half, k=k):
                own = at(i * CHUNK, CHUNK, CHUNK)
                here = at(base + i * CHUNK, CHUNK, CHUNK)
                when = at(half + i * CHUNK, CHUNK, CHUNK)
                coded = block[own, at(F + c * W, W, W)].astype(F32) + block[
                    own, at(F + 2 * W + c * W, W, W)
                ].astype(F32)
                same = coded < 1.5
                prior = jnp.where(same, coded, 0.0)
                gz = jax.nn.sigmoid(pre[here, 0:W] + rz * prior + bz)
                gr = jax.nn.sigmoid(pre[here, W : 2 * W] + rr * prior + br)
                reset = gr * prior
                gc = jnp.tanh(pre[here, 2 * W : 3 * W] + rc * reset + bc)
                keep = 1.0 - gz
                fz = (gc - prior) * gz * keep
                fc = gz * (1.0 - gc * gc)
                side_r = prior * gr * (1.0 - gr)
                value = keep + fz * rz + fc * rc * (gr + side_r * rr)
                jac[k, when, :] = jnp.where(same, value, 0.0)
                upg[k, when, :] = block[own, at(F + 4 * W + c * W, W, W)].astype(F32)
                az[here, :] = fz
                ac[here, :] = fc
                ar[here, :] = fc * rc * side_r
                pr[here, :] = prior
                rp[here, :] = reset
                return carry

            lax.fori_loop(0, T // CHUNK, step, 0)
    sub = lax.broadcasted_iota(jnp.int32, (8, 8, W), 1)
    for k in range(4):
        for n in range(4):
            f = jac[k, n * 64 + 1 : n * 64 + 65, :].reshape(8, 8, W)
            a = upg[k, n * 64 : n * 64 + 64, :].reshape(8, 8, W)
            for d in (1, 2, 4):
                valid = sub < 8 - d
                a = jnp.where(valid, a + f * pltpu.roll(a, 8 - d, 1), a)
                f = jnp.where(valid, f * pltpu.roll(f, 8 - d, 1), f)
            loc[k * 256 + n * 64 : k * 256 + n * 64 + 64, :] = a.reshape(64, W)
            fac[k * 256 + n * 64 : k * 256 + n * 64 + 64, :] = f.reshape(64, W)

    def chain(i, carry):
        new = []
        for k in range(4):
            a0, f0 = carry[2 * k], carry[2 * k + 1]
            here = at(k * 256 + (31 - i) * 8, 8, 8)
            f = fac[here, :]
            a = loc[here, :] + f * a0
            f = f * f0
            loc[here, :] = a
            fac[here, :] = f
            new += [jnp.broadcast_to(a[0:1], (8, W)), jnp.broadcast_to(f[0:1], (8, W))]
        return tuple(new)

    start = (jnp.zeros((8, W), F32), jnp.ones((8, W), F32)) * 4
    last = lax.fori_loop(0, 32, chain, start, unroll=4)
    for k in range(4):
        ends[k : k + 1, :] = jac[k, 0:1, :] * last[2 * k + 1][0:1]
        ends[4 + k : 5 + k, :] = jac[k, 0:1, :] * last[2 * k][0:1]


def backward_body(idx, one, two, az, ac, ar, pr, rp, loc, fac, *refs):
    blocks, refs = refs[:8], refs[8:]
    grads, own, own_stats, *rest = refs
    sent, total = rest[:3], rest[3]
    y, c = idx[1], idx[2]
    enter = one[4:8, :] + one[0:4, :] * two[4:8, :]
    sums = (jnp.zeros((8, W), F32),) * 6
    for k in range(4):
        came = enter[k : k + 1]
        for side in range(2):
            base = k * 256 + side * T
            half = k * 256 + lax.rem(c + side, 2) * T

            def step(i, sums, base=base, half=half, came=came):
                here = at(base + i * CHUNK, CHUNK, CHUNK)
                when = at(half + i * CHUNK, CHUNK, CHUNK)
                adj = loc[when, :] + fac[when, :] * came
                gz, gc, gr = adj * az[here, :], adj * ac[here, :], adj * ar[here, :]
                prior = pr[here, :]
                grads[here, 0:W] = gz.astype(BF)
                grads[here, W : 2 * W] = gr.astype(BF)
                grads[here, 2 * W : 3 * W] = gc.astype(BF)
                terms = (gz, gr, gc, gz * prior, gr * prior, gc * rp[here, :])
                return tuple(s + t.reshape(CHUNK // 8, 8, W).sum(0) for s, t in zip(sums, terms))

            sums = lax.fori_loop(0, T // CHUNK, step, sums)
    own_stats[...] = jnp.zeros((8, W), F32)
    for n in range(6):
        own_stats[n : n + 1, :] = jnp.sum(sums[n], 0, keepdims=True)
    feats = jnp.concatenate([b[:, 0:F] for k in range(4) for b in (blocks[k], blocks[4 + k])], 0)
    whole = lax.dot_general(
        grads[...], feats, (((0,), (0,)), ((), ())), preferred_element_type=F32
    )
    for b in range(4):
        total[b] = whole[:, b * CB : (b + 1) * CB]
    own[...] = total[y]
    for k in range(1, 4):
        sent[k - 1][0:384, :] = total[lax.rem(y + k, NY)].astype(BF)
        put_stats(sent[k - 1], 384, own_stats[...])


def put_stats(ref, row, stats):
    pair = jnp.concatenate([stats, jnp.zeros_like(stats)], 0)
    high, low = split2(pair)
    ref[row : row + 16, 0:W] = high
    ref[row : row + 16, W : 2 * W] = low


def get_stats(ref, row):
    both = ref[row : row + 16, 0:W].astype(F32) + ref[row : row + 16, W : 2 * W].astype(F32)
    return both[0:8]


def input_grad_body(idx, grads, weight, mine, other):
    rows = jnp.concatenate([weight[b] for b in range(4)], 1)
    for k in range(4):
        part = jnp.dot(grads[k * 256 : k * 256 + 256, :], rows, preferred_element_type=F32)
        mine[k] = part[0:T]
        other[k] = part[T : 2 * T].astype(BF)


def core_sum_body(idx, mine, other, own, *sent):
    own[...] = mine[0] + other[0].astype(F32)
    for k in range(1, 4):
        sent[k - 1][...] = (mine[k] + other[k].astype(F32)).astype(BF)


def block_sum_body(idx, own, *refs):
    *came, out = refs
    out[...] = (own[...] + sum(r[...].astype(F32) for r in came)).astype(BF)


def y_sum_body(idx, own, own_stats, *refs):
    came, refs = refs[:3], refs[3:]
    piece, stats, *sent = refs[:9]
    total = refs[9]
    z = idx[0]
    total[...] = own[...] + sum(r[0:384, :].astype(F32) for r in came)
    stats[...] = own_stats[...] + sum(get_stats(r, 384) for r in came)
    for k in range(8):
        unit = lax.rem(z + k, NZ)
        for g in range(3):
            rows = total[at(g * W + unit * UNIT, UNIT, UNIT), :]
            if k == 0:
                piece[g * UNIT : (g + 1) * UNIT, :] = rows
            else:
                sent[k - 1][g * UNIT : (g + 1) * UNIT, :] = rows.astype(BF)
        if k:
            put_stats(sent[k - 1], 48, stats[...])


def z_sum_body(scale, idx, piece, stats, *refs):
    came, refs = refs[:7], refs[7:]
    outs, stats_out, total = refs[:3], refs[3], refs[4]
    z, c, x = idx[0], idx[2], idx[3]
    total[...] = (piece[...] + sum(r[0:48, :].astype(F32) for r in came)) * scale
    stats_out[...] = (stats[...] + sum(get_stats(r, 48) for r in came)) * scale
    hidden = (c * 4 + x) * 8 + z
    for k in range(3):
        gate = lax.rem(k + 3 - lax.rem(hidden, 3), 3)
        outs[k][...] = total[at(gate * UNIT, UNIT, UNIT), :]


def stats_body(idx, *refs):
    came, out, table = refs[:4], refs[4], refs[5]
    c, x = idx[2], idx[3]
    for k in range(4):
        for side in range(2):
            place = lax.rem(c + side, 2) * 4 + lax.rem(x - k + 4, 4)
            table[place] = came[k][side * 8 : side * 8 + 8, :]
    for n in range(8):
        out[:, n * W : (n + 1) * W] = table[n][0:6]


def local(inputs, weight_t, states, doc_ids, recur, bias, out_grad):
    device = lax.axis_index(ALL)
    sizes = jnp.array([NZ, NY, NC, NX], jnp.int32)
    idx = (device // jnp.array([32, 8, 4, 1], jnp.int32)) % sizes
    states, out_grad = states[0], out_grad[0]

    pieces = [
        lax.ppermute(weight_t[k * UNIT : (k + 1) * UNIT], ALL, piece_route(k)) for k in range(3)
    ]
    pieces = jnp.concatenate(pieces, 0)
    column = jnp.concatenate([pieces] + [around(pieces, "z", k) for k in range(1, NZ)], 0)
    parts = [column] + [around(column, "y", k) for k in range(1, NY)]

    ids = doc_ids[0].astype(F32)
    tail = jnp.concatenate([states[-1:], jnp.broadcast_to(ids[-1:], (1, H))], 0)
    tail = along(tail, SEQ, NZ * NY * NC, 1)
    ids = jnp.broadcast_to(ids[:, None], (T, W))
    sent = call(
        messages_body,
        [((T, MSG), BF)] * 4,
        (idx, inputs[0], states, ids, out_grad, tail),
        name="messages",
    )
    mine = [sent[0]] + [around(sent[k], "x", k) for k in range(1, NX)]
    other = [around(m, "c", 1) for m in mine]
    blocks = mine + other

    tokens = ((8 * T, W), F32)
    *kept, ends, weight = call(
        forward_body,
        [tokens] * 7 + [((8, W), F32), ((4, 3 * W, CB), BF)],
        (idx, recur, bias, *blocks, *parts),
        [
            pltpu.VMEM((8 * T, 3 * W), F32),
            pltpu.VMEM((4, 2 * T + 8, W), F32),
            pltpu.VMEM((4, 2 * T, W), F32),
        ],
        name="forward",
    )
    one = along(ends, ("z", "y"), NZ * NY, -1)
    two = along(ends, ("z", "y"), NZ * NY, -2)
    grads, own, stats, *sent = call(
        backward_body,
        [((8 * T, 3 * W), BF), ((3 * W, CB), F32), ((8, W), F32)] + [((400, CB), BF)] * 3,
        (idx, one, two, *kept, *blocks),
        [pltpu.VMEM((4, 3 * W, CB), F32)],
        name="backward",
    )
    came = [around(sent[k - 1], "y", k) for k in range(1, NY)]

    mine, other = call(
        input_grad_body,
        [((4, T, F), F32), ((4, T, F), BF)],
        (idx, grads, weight),
        name="input_grad",
    )
    other = around(other, "c", 1)
    block, *back = call(
        core_sum_body,
        [((T, F), F32)] + [((T, F), BF)] * 3,
        (idx, mine, other),
        name="core_sum",
    )
    back = [around(back[k - 1], "x", NX - k) for k in range(1, NX)]

    piece, stats, *sent = call(
        y_sum_body,
        [((48, CB), F32), ((8, W), F32)] + [((64, CB), BF)] * 7,
        (idx, own, stats, *came),
        [pltpu.VMEM((3 * W, CB), F32)],
        name="y_sum",
    )
    came = [around(sent[k - 1], "z", k) for k in range(1, NZ)]
    scale = 1.0 / math.sqrt(inputs.shape[0] * T * NZ * NY * NC * NX)
    *pieces, stats = call(
        functools.partial(z_sum_body, scale),
        [((UNIT, CB), F32)] * 3 + [((8, W), F32)],
        (idx, piece, stats, *came),
        [pltpu.VMEM((48, CB), F32)],
        name="z_sum",
    )
    pieces = [
        lax.ppermute(pieces[k], ALL, [(b, a) for a, b in piece_route(k)]) for k in range(3)
    ]
    weight_grad = jnp.concatenate(pieces, 0)
    stats = jnp.concatenate([stats, around(stats, "c", 1)], 0)
    stats = [stats] + [around(stats, "x", k) for k in range(1, NX)]
    (param_grad,) = call(
        stats_body,
        [((6, H), F32)],
        (idx, *stats),
        [pltpu.VMEM((8, 8, W), F32)],
        name="stats",
    )
    (input_grad,) = call(block_sum_body, [((T, F), BF)], (idx, block, *back), name="block_sum")
    return input_grad[None], weight_grad, param_grad


def solution(mesh):
    torus = Mesh(mesh.devices.reshape(NZ, NY, NC, NX), ALL)
    in_specs = (
        P("x", SEQ, None),
        P(SEQ, "x"),
        P("x", SEQ, None),
        P("x", SEQ),
        P(),
        P(),
        P("x", SEQ, None),
    )
    out_specs = (P("x", SEQ, None), P(SEQ, "x"), P())
    return jax.shard_map(local, mesh=torus, in_specs=in_specs, out_specs=out_specs, check_vma=False)
```

```python
import functools
import math

import jax
import jax.numpy as jnp
from jax import lax
from jax.experimental import pallas as pl
from jax.experimental.pallas import tpu as pltpu
from jax.sharding import Mesh
from jax.sharding import PartitionSpec as P

SEQ = ("z", "y", "c")
ALL = ("z", "y", "c", "x")
NZ, NY, NC, NX = 8, 4, 2, 4
T = 128
F = 1024
H = 1024
W = 128
UNIT = 16
CB = F // 4
FAR = 2.0
CHUNK = 32
BF = jnp.bfloat16
F32 = jnp.float32


def around(a, axis, k):
    n = lax.axis_size(axis)
    return lax.ppermute(a, axis, [(i, (i + k) % n) for i in range(n)])


def exchange(a, axes):
    return lax.all_to_all(a, axes, split_axis=0, concat_axis=0, tiled=True)


def place(share, yc, k):
    plane = lax.rem(3 * (share + 8 - ((3 * yc + k) >> 3)), 8)
    unit = 24 * plane + 3 * yc + k
    return plane, unit >> 6, unit & 7


def along(a, axis, n, k):
    return lax.ppermute(a, axis, [(i, i + k) for i in range(n) if 0 <= i + k < n])


def call(body, outs, args, scratch=(), name=None):
    vmem = pl.BlockSpec(memory_space=pltpu.VMEM)
    return pl.pallas_call(
        body,
        out_shape=[jax.ShapeDtypeStruct(s, d) for s, d in outs],
        in_specs=[pl.BlockSpec(memory_space=pltpu.SMEM)] + [vmem] * (len(args) - 1),
        out_specs=[vmem] * len(outs),
        scratch_shapes=list(scratch),
        name=name,
    )(*args)


def at(start, size, step):
    return pl.ds(pl.multiple_of(start, step), size)


def split2(v):
    high = v.astype(BF)
    return high, (v - high.astype(F32)).astype(BF)


MSG = F + 3 * 2 * W


def messages_body(idx, inputs, states, ids, grads, tail, *outs):
    first = (idx[0] == 0) & (idx[1] == 0) & (idx[2] == 0)
    row = lax.broadcasted_iota(jnp.int32, (T, W), 0)
    before = jnp.where(row == 0, tail[1:2, 0:W], pltpu.roll(ids[...], 1, 0))
    same = (before == ids[...]) & ((row > 0) | jnp.logical_not(first))
    for k in range(NX):
        out = outs[k]
        x = lax.rem(idx[3] + k, NX)
        out[:, 0:F] = inputs[...]
        for c in range(NC):
            lanes = at(c * 512 + x * W, W, W)
            prior = jnp.where(row == 0, tail[0:1, lanes], pltpu.roll(states[:, lanes], 1, 0))
            high, low = split2(jnp.where(same, prior, FAR))
            out[:, F + c * W : F + (c + 1) * W] = high
            out[:, F + (2 + c) * W : F + (3 + c) * W] = low
            out[:, F + (4 + c) * W : F + (5 + c) * W] = grads[:, lanes]


def choose_body(idx, column, out):
    yc = idx[1] * NC + idx[2]
    for share in range(8):
        for k in range(3):
            plane, _, _ = place(share, yc, k)
            rows = column[plane, k * UNIT : (k + 1) * UNIT, :]
            for y in range(NY):
                out[y * 8 + share, k * UNIT : (k + 1) * UNIT, :] = rows


def forward_body(idx, recur, bias, *refs):
    mine, other, parts, *refs = refs[:4], refs[4:8], *refs[8:]
    az, ac, ar, pr, rp, loc, fac, ends, weight, pre, jac, upg = refs
    c, x = idx[2], idx[3]
    share = c * 4 + x
    for yc in range(NY * NC):
        for k in range(3):
            _, gate, unit = place(share, yc, k)
            rows = at(gate * W + unit * UNIT, UNIT, UNIT)
            for b in range(NX):
                weight[b, rows, :] = parts[yc * NX + b, k * UNIT : (k + 1) * UNIT, :]
    feats = jnp.concatenate([b[k][:, 0:F] for k in range(4) for b in (mine, other)], 0)
    rows = jnp.concatenate([weight[b] for b in range(4)], 1)
    pre[...] = lax.dot_general(feats, rows, (((1,), (1,)), ((), ())), preferred_element_type=F32)
    lanes = at(share * W, W, W)
    rz, rr, rc = (recur[g : g + 1, lanes] for g in range(3))
    bz, br, bc = (bias[g : g + 1, lanes] for g in range(3))
    for k in range(4):
        jac[k, 2 * T : 2 * T + 8, :] = jnp.ones((8, W), F32)
        for side in range(2):
            block = (other if side else mine)[k]
            base = k * 256 + side * T
            half = lax.rem(c + side, 2) * T

            def step(i, carry, block=block, base=base, half=half, k=k):
                own = at(i * CHUNK, CHUNK, CHUNK)
                here = at(base + i * CHUNK, CHUNK, CHUNK)
                when = at(half + i * CHUNK, CHUNK, CHUNK)
                coded = block[own, at(F + c * W, W, W)].astype(F32) + block[
                    own, at(F + 2 * W + c * W, W, W)
                ].astype(F32)
                same = coded < 1.5
                prior = jnp.where(same, coded, 0.0)
                gz = jax.nn.sigmoid(pre[here, 0:W] + rz * prior + bz)
                gr = jax.nn.sigmoid(pre[here, W : 2 * W] + rr * prior + br)
                reset = gr * prior
                gc = jnp.tanh(pre[here, 2 * W : 3 * W] + rc * reset + bc)
                keep = 1.0 - gz
                fz = (gc - prior) * gz * keep
                fc = gz * (1.0 - gc * gc)
                side_r = prior * gr * (1.0 - gr)
                value = keep + fz * rz + fc * rc * (gr + side_r * rr)
                jac[k, when, :] = jnp.where(same, value, 0.0)
                upg[k, when, :] = block[own, at(F + 4 * W + c * W, W, W)].astype(F32)
                az[here, :] = fz
                ac[here, :] = fc
                ar[here, :] = fc * rc * side_r
                pr[here, :] = prior
                rp[here, :] = reset
                return carry

            lax.fori_loop(0, T // CHUNK, step, 0)
    sub = lax.broadcasted_iota(jnp.int32, (8, 8, W), 1)
    for k in range(4):
        for n in range(4):
            f = jac[k, n * 64 + 1 : n * 64 + 65, :].reshape(8, 8, W)
            a = upg[k, n * 64 : n * 64 + 64, :].reshape(8, 8, W)
            for d in (1, 2, 4):
                valid = sub < 8 - d
                a = jnp.where(valid, a + f * pltpu.roll(a, 8 - d, 1), a)
                f = jnp.where(valid, f * pltpu.roll(f, 8 - d, 1), f)
            loc[k * 256 + n * 64 : k * 256 + n * 64 + 64, :] = a.reshape(64, W)
            fac[k * 256 + n * 64 : k * 256 + n * 64 + 64, :] = f.reshape(64, W)

    def chain(i, carry):
        new = []
        for k in range(4):
            a0, f0 = carry[2 * k], carry[2 * k + 1]
            here = at(k * 256 + (31 - i) * 8, 8, 8)
            f = fac[here, :]
            a = loc[here, :] + f * a0
            f = f * f0
            loc[here, :] = a
            fac[here, :] = f
            new += [jnp.broadcast_to(a[0:1], (8, W)), jnp.broadcast_to(f[0:1], (8, W))]
        return tuple(new)

    start = (jnp.zeros((8, W), F32), jnp.ones((8, W), F32)) * 4
    last = lax.fori_loop(0, 32, chain, start, unroll=4)
    for k in range(4):
        ends[k : k + 1, :] = jac[k, 0:1, :] * last[2 * k + 1][0:1]
        ends[4 + k : 5 + k, :] = jac[k, 0:1, :] * last[2 * k][0:1]


def backward_body(idx, one, two, az, ac, ar, pr, rp, loc, fac, *refs):
    mine, other, grads, sent, total = refs[:4], refs[4:8], *refs[8:]
    c = idx[2]
    share = c * 4 + idx[3]
    enter = one[4:8, :] + one[0:4, :] * two[4:8, :]
    sums = (jnp.zeros((8, W), F32),) * 6
    for k in range(4):
        came = enter[k : k + 1]
        for side in range(2):
            base = k * 256 + side * T
            half = k * 256 + lax.rem(c + side, 2) * T

            def step(i, sums, base=base, half=half, came=came):
                here = at(base + i * CHUNK, CHUNK, CHUNK)
                when = at(half + i * CHUNK, CHUNK, CHUNK)
                adj = loc[when, :] + fac[when, :] * came
                gz, gc, gr = adj * az[here, :], adj * ac[here, :], adj * ar[here, :]
                prior = pr[here, :]
                grads[here, 0:W] = gz.astype(BF)
                grads[here, W : 2 * W] = gr.astype(BF)
                grads[here, 2 * W : 3 * W] = gc.astype(BF)
                terms = (gz, gr, gc, gz * prior, gr * prior, gc * rp[here, :])
                return tuple(s + t.reshape(CHUNK // 8, 8, W).sum(0) for s, t in zip(sums, terms))

            sums = lax.fori_loop(0, T // CHUNK, step, sums)
    feats = jnp.concatenate([b[k][:, 0:F] for k in range(4) for b in (mine, other)], 0)
    whole = lax.dot_general(
        grads[...], feats, (((0,), (0,)), ((), ())), preferred_element_type=F32
    )
    for b in range(4):
        total[b] = whole[:, b * CB : (b + 1) * CB]
    stats = jnp.concatenate([jnp.sum(s, 0, keepdims=True) for s in sums], 0)
    high, low = split2(jnp.concatenate([stats, jnp.zeros((10, W), F32)], 0))
    for yc in range(NY * NC):
        for k in range(3):
            _, gate, unit = place(share, yc, k)
            rows = at(gate * W + unit * UNIT, UNIT, UNIT)
            for b in range(NX):
                piece = total[b, rows, :].astype(BF)
                sent[yc * NX + b, k * UNIT : (k + 1) * UNIT, :] = piece
        for b in range(NX):
            sent[yc * NX + b, 48:64, 0:W] = high
            sent[yc * NX + b, 48:64, W : 2 * W] = low


def input_grad_body(idx, grads, weight, mine, other):
    rows = jnp.concatenate([weight[b] for b in range(4)], 1)
    for k in range(4):
        part = jnp.dot(grads[k * 256 : k * 256 + 256, :], rows, preferred_element_type=F32)
        mine[k] = part[0:T]
        other[k] = part[T : 2 * T].astype(BF)


def core_sum_body(idx, mine, other, own, *sent):
    own[...] = mine[0] + other[0].astype(F32)
    for k in range(1, NX):
        sent[k - 1][...] = (mine[k] + other[k].astype(F32)).astype(BF)


def block_sum_body(idx, own, *refs):
    *came, out = refs
    out[...] = (own[...] + sum(r[...].astype(F32) for r in came)).astype(BF)


def y_sum_body(idx, came, piece, stats, sent, total):
    yc = idx[1] * NC + idx[2]
    for share in range(8):
        rows = sum(came[y * 8 + share].astype(F32) for y in range(NY))
        for k in range(3):
            plane, _, _ = place(share, yc, k)
            total[plane, k * UNIT : (k + 1) * UNIT, :] = rows[k * UNIT : (k + 1) * UNIT]
        lanes = slice(share * W, share * W + W)
        stats[:, lanes] = rows[48:56, 0:W] + rows[48:56, W : 2 * W]
    lines = jnp.concatenate([stats[:, b * CB : (b + 1) * CB] for b in range(4)], 0).astype(BF)
    for z in range(NZ):
        sent[z, 0:48, :] = total[z].astype(BF)
        sent[z, 48:80, :] = lines
    piece[...] = total[idx[0]]


def z_sum_body(scale, idx, piece, stats, came, weight_grad, param_grad):
    rows = sum(came[lax.rem(idx[0] + k, NZ)].astype(F32) for k in range(1, NZ))
    weight_grad[...] = (piece[...] + rows[0:48]) * scale
    for b in range(4):
        lanes = slice(b * CB, (b + 1) * CB)
        param_grad[:, lanes] = (stats[0:6, lanes] + rows[48 + b * 8 : 54 + b * 8]) * scale


def local(inputs, weight_t, states, doc_ids, recur, bias, out_grad):
    device = lax.axis_index(ALL)
    sizes = jnp.array([NZ, NY, NC, NX], jnp.int32)
    idx = (device // jnp.array([32, 8, 4, 1], jnp.int32)) % sizes
    states, out_grad = states[0], out_grad[0]
    plane = ("y", "c", "x")

    ids = doc_ids[0].astype(F32)
    tail = jnp.concatenate([states[-1:], jnp.broadcast_to(ids[-1:], (1, H))], 0)
    tail = along(tail, SEQ, NZ * NY * NC, 1)
    ids = jnp.broadcast_to(ids[:, None], (T, W))
    sent = call(
        messages_body,
        [((T, MSG), BF)] * NX,
        (idx, inputs[0], states, ids, out_grad, tail),
        name="messages",
    )
    mine = [sent[0]] + [around(sent[k], "x", k) for k in range(1, NX)]
    blocks = mine + [around(m, "c", 1) for m in mine]

    column = exchange(jnp.broadcast_to(weight_t, (NZ, 48, CB)), "z")
    (parts,) = call(choose_body, [((32, 48, CB), BF)], (idx, column), name="choose")
    parts = exchange(parts, plane)

    tokens = ((8 * T, W), F32)
    *kept, ends, weight = call(
        forward_body,
        [tokens] * 7 + [((8, W), F32), ((4, 3 * W, CB), BF)],
        (idx, recur, bias, *blocks, parts),
        [
            pltpu.VMEM((8 * T, 3 * W), F32),
            pltpu.VMEM((4, 2 * T + 8, W), F32),
            pltpu.VMEM((4, 2 * T, W), F32),
        ],
        name="forward",
    )
    one = along(ends, ("z", "y"), NZ * NY, -1)
    two = along(ends, ("z", "y"), NZ * NY, -2)
    grads, sent = call(
        backward_body,
        [((8 * T, 3 * W), BF), ((32, 64, CB), BF)],
        (idx, one, two, *kept, *blocks),
        [pltpu.VMEM((4, 3 * W, CB), F32)],
        name="backward",
    )

    came = exchange(sent, plane)
    piece, stats, sent = call(
        y_sum_body,
        [((48, CB), F32), ((8, H), F32), ((NZ, 80, CB), BF)],
        (idx, came),
        [pltpu.VMEM((NZ, 48, CB), F32)],
        name="y_sum",
    )
    came = exchange(sent, "z")
    scale = 1.0 / math.sqrt(inputs.shape[0] * T * NZ * NY * NC * NX)
    weight_grad, param_grad = call(
        functools.partial(z_sum_body, scale),
        [((48, CB), F32), ((6, H), F32)],
        (idx, piece, stats, came),
        name="z_sum",
    )

    mine, other = call(
        input_grad_body,
        [((4, T, F), F32), ((4, T, F), BF)],
        (idx, grads, weight),
        name="input_grad",
    )
    other = lax.ppermute(other, "c", [(0, 1), (1, 0)])
    own, *sent = call(
        core_sum_body,
        [((T, F), F32)] + [((T, F), BF)] * 3,
        (idx, mine, other),
        name="core_sum",
    )
    came = [around(sent[k - 1], "x", NX - k) for k in range(1, NX)]
    (input_grad,) = call(block_sum_body, [((T, F), BF)], (idx, own, *came), name="block_sum")
    return input_grad[None], weight_grad, param_grad


def solution(mesh):
    torus = Mesh(mesh.devices.reshape(NZ, NY, NC, NX), ALL)
    in_specs = (
        P("x", SEQ, None),
        P(SEQ, "x"),
        P("x", SEQ, None),
        P("x", SEQ),
        P(),
        P(),
        P("x", SEQ, None),
    )
    out_specs = (P("x", SEQ, None), P(SEQ, "x"), P())
    return jax.shard_map(local, mesh=torus, in_specs=in_specs, out_specs=out_specs, check_vma=False)
```

```python
import functools
import math

import jax
import jax.numpy as jnp
from jax import lax
from jax.experimental import pallas as pl
from jax.experimental.pallas import tpu as pltpu
from jax.sharding import Mesh
from jax.sharding import PartitionSpec as P

SEQ = ("z", "y", "c")
ALL = ("z", "y", "c", "x")
NZ, NY, NC, NX = 8, 4, 2, 4
T = 128
F = 1024
H = 1024
W = 128
UNIT = 16
CB = F // 4
FAR = 2.0
CHUNK = 32
BF = jnp.bfloat16
F32 = jnp.float32


def around(a, axis, k):
    n = lax.axis_size(axis)
    return lax.ppermute(a, axis, [(i, (i + k) % n) for i in range(n)])


def exchange(a, axes):
    return lax.all_to_all(a, axes, split_axis=0, concat_axis=0, tiled=True)


def place(share, yc, k):
    plane = lax.rem(3 * (share + 8 - ((3 * yc + k) >> 3)), 8)
    unit = 24 * plane + 3 * yc + k
    return plane, unit >> 6, unit & 7


def along(a, axis, n, k):
    return lax.ppermute(a, axis, [(i, i + k) for i in range(n) if 0 <= i + k < n])


def call(body, outs, args, scratch=()):
    vmem = pl.BlockSpec(memory_space=pltpu.VMEM)
    return pl.pallas_call(
        body,
        out_shape=[jax.ShapeDtypeStruct(s, d) for s, d in outs],
        in_specs=[pl.BlockSpec(memory_space=pltpu.SMEM)] + [vmem] * (len(args) - 1),
        out_specs=[vmem] * len(outs),
        scratch_shapes=list(scratch),
    )(*args)


def coords(idx):
    n = idx[0]
    return n >> 5, (n >> 3) & 3, (n >> 2) & 1, n & 3


def at(start, size, step):
    return pl.ds(pl.multiple_of(start, step), size)


def split2(v):
    high = v.astype(BF)
    return high, (v - high.astype(F32)).astype(BF)


MSG = F + 2 * 2 * W


def prepare_body(weight, states, ids, copies, tail):
    for z in range(NZ):
        copies[z] = weight[...]
    tail[0:1, :] = states[7:8, :]
    tail[1:2, :] = jnp.broadcast_to(ids[0:1, T - 1 : T].astype(F32), (1, H))


def messages_body(idx, inputs, states, ids, grads, tail, *outs):
    z, y, c, x_own = coords(idx)
    row = lax.broadcasted_iota(jnp.int32, (T, W), 0)
    lane = lax.broadcasted_iota(jnp.int32, (T, W), 1)
    number = ids[...].astype(F32)
    column = jnp.sum(jnp.where(row == lane, number, 0.0), 1, keepdims=True)
    column = jnp.broadcast_to(column, (T, W))
    before = jnp.where(row == 0, tail[1:2, 0:W], pltpu.roll(column, 1, 0))
    same = (before == column) & ((row > 0) | (z + y + c > 0))
    for k in range(NX):
        out = outs[k]
        x = lax.rem(x_own + k, NX)
        out[:, 0:F] = inputs[...]
        for c in range(NC):
            lanes = at(c * 512 + x * W, W, W)
            prior = jnp.where(row == 0, tail[0:1, lanes], pltpu.roll(states[:, lanes], 1, 0))
            out[:, F + c * W : F + (c + 1) * W] = jnp.where(same, prior, FAR).astype(BF)
            out[:, F + (2 + c) * W : F + (3 + c) * W] = grads[:, lanes]


def choose_body(idx, column, out):
    _, y, c, _ = coords(idx)
    yc = y * NC + c
    for share in range(8):
        for k in range(3):
            plane, _, _ = place(share, yc, k)
            rows = column[plane, k * UNIT : (k + 1) * UNIT, :]
            for to in range(NY):
                out[to * 8 + share, k * UNIT : (k + 1) * UNIT, :] = rows


def forward_body(idx, recur, bias, *refs):
    mine, other, parts, *refs = refs[:4], refs[4:8], *refs[8:]
    az, ac, ar, pr, rp, loc, fac, ends, weight, pre, jac, upg = refs
    _, _, c, x = coords(idx)
    share = c * 4 + x
    for yc in range(NY * NC):
        for k in range(3):
            _, gate, unit = place(share, yc, k)
            rows = at(gate * W + unit * UNIT, UNIT, UNIT)
            for b in range(NX):
                weight[b, rows, :] = parts[yc * NX + b, k * UNIT : (k + 1) * UNIT, :]
    feats = jnp.concatenate([b[k][:, 0:F] for k in range(4) for b in (mine, other)], 0)
    rows = jnp.concatenate([weight[b] for b in range(4)], 1)
    pre[...] = lax.dot_general(feats, rows, (((1,), (1,)), ((), ())), preferred_element_type=F32)
    lanes = at(share * W, W, W)
    rz, rr, rc = (recur[g : g + 1, lanes] for g in range(3))
    bz, br, bc = (bias[g : g + 1, lanes] for g in range(3))
    for k in range(4):
        jac[k, 2 * T : 2 * T + 8, :] = jnp.ones((8, W), F32)
        for side in range(2):
            block = (other if side else mine)[k]
            base = k * 256 + side * T
            half = lax.rem(c + side, 2) * T

            def step(i, carry, block=block, base=base, half=half, k=k):
                own = at(i * CHUNK, CHUNK, CHUNK)
                here = at(base + i * CHUNK, CHUNK, CHUNK)
                when = at(half + i * CHUNK, CHUNK, CHUNK)
                coded = block[own, at(F + c * W, W, W)].astype(F32)
                same = coded < 1.5
                prior = jnp.where(same, coded, 0.0)
                gz = jax.nn.sigmoid(pre[here, 0:W] + rz * prior + bz)
                gr = jax.nn.sigmoid(pre[here, W : 2 * W] + rr * prior + br)
                reset = gr * prior
                gc = jnp.tanh(pre[here, 2 * W : 3 * W] + rc * reset + bc)
                keep = 1.0 - gz
                fz = (gc - prior) * gz * keep
                fc = gz * (1.0 - gc * gc)
                side_r = prior * gr * (1.0 - gr)
                value = keep + fz * rz + fc * rc * (gr + side_r * rr)
                jac[k, when, :] = jnp.where(same, value, 0.0)
                upg[k, when, :] = block[own, at(F + 2 * W + c * W, W, W)].astype(F32)
                az[here, :] = fz
                ac[here, :] = fc
                ar[here, :] = fc * rc * side_r
                pr[here, :] = prior
                rp[here, :] = reset
                return carry

            lax.fori_loop(0, T // CHUNK, step, 0)
    sub = lax.broadcasted_iota(jnp.int32, (8, 8, W), 1)
    for k in range(4):
        for n in range(4):
            f = jac[k, n * 64 + 1 : n * 64 + 65, :].reshape(8, 8, W)
            a = upg[k, n * 64 : n * 64 + 64, :].reshape(8, 8, W)
            for d in (1, 2, 4):
                valid = sub < 8 - d
                a = jnp.where(valid, a + f * pltpu.roll(a, 8 - d, 1), a)
                f = jnp.where(valid, f * pltpu.roll(f, 8 - d, 1), f)
            loc[k * 256 + n * 64 : k * 256 + n * 64 + 64, :] = a.reshape(64, W)
            fac[k * 256 + n * 64 : k * 256 + n * 64 + 64, :] = f.reshape(64, W)

    def chain(i, carry):
        new = []
        for k in range(4):
            a0, f0 = carry[2 * k], carry[2 * k + 1]
            here = at(k * 256 + (31 - i) * 8, 8, 8)
            f = fac[here, :]
            a = loc[here, :] + f * a0
            f = f * f0
            loc[here, :] = a
            fac[here, :] = f
            new += [jnp.broadcast_to(a[0:1], (8, W)), jnp.broadcast_to(f[0:1], (8, W))]
        return tuple(new)

    start = (jnp.zeros((8, W), F32), jnp.ones((8, W), F32)) * 4
    last = lax.fori_loop(0, 32, chain, start, unroll=4)
    for k in range(4):
        ends[k : k + 1, :] = jac[k, 0:1, :] * last[2 * k + 1][0:1]
        ends[4 + k : 5 + k, :] = jac[k, 0:1, :] * last[2 * k][0:1]


def backward_body(idx, one, two, az, ac, ar, pr, rp, loc, fac, *refs):
    mine, other, near, far, sent, total = refs[:4], refs[4:8], *refs[8:]
    _, _, c, x = coords(idx)
    share = c * 4 + x
    enter = one[4:8, :] + one[0:4, :] * two[4:8, :]
    sums = (jnp.zeros((8, W), F32),) * 6
    for k in range(4):
        came = enter[k : k + 1]
        for side in range(2):
            base = k * 256 + side * T
            half = k * 256 + lax.rem(c + side, 2) * T
            grads = far if side else near

            def step(i, sums, base=base, half=half, came=came, k=k, grads=grads):
                here = at(base + i * CHUNK, CHUNK, CHUNK)
                when = at(half + i * CHUNK, CHUNK, CHUNK)
                adj = loc[when, :] + fac[when, :] * came
                gz, gc, gr = adj * az[here, :], adj * ac[here, :], adj * ar[here, :]
                prior = pr[here, :]
                rows = at(k * T + i * CHUNK, CHUNK, CHUNK)
                grads[rows, 0:W] = gz.astype(BF)
                grads[rows, W : 2 * W] = gr.astype(BF)
                grads[rows, 2 * W : 3 * W] = gc.astype(BF)
                terms = (gz, gr, gc, gz * prior, gr * prior, gc * rp[here, :])
                return tuple(s + t.reshape(CHUNK // 8, 8, W).sum(0) for s, t in zip(sums, terms))

            sums = lax.fori_loop(0, T // CHUNK, step, sums)
    feats = jnp.concatenate([b[:, 0:F] for b in (*mine, *other)], 0)
    grads = jnp.concatenate([near[...], far[...]], 0)
    whole = lax.dot_general(grads, feats, (((0,), (0,)), ((), ())), preferred_element_type=F32)
    for b in range(4):
        total[b] = whole[:, b * CB : (b + 1) * CB]
    stats = jnp.concatenate([jnp.sum(s, 0, keepdims=True) for s in sums], 0)
    high, low = split2(jnp.concatenate([stats, jnp.zeros((2, W), F32)], 0))
    for yc in range(NY * NC):
        for k in range(3):
            _, gate, unit = place(share, yc, k)
            rows = at(gate * W + unit * UNIT, UNIT, UNIT)
            for b in range(NX):
                piece = total[b, rows, :].astype(BF)
                sent[yc * NX + b, k * UNIT : (k + 1) * UNIT, :] = piece
        for b in range(NX):
            sent[yc * NX + b, 48:56, 0:W] = high
            sent[yc * NX + b, 48:56, W : 2 * W] = low


def input_grad_body(idx, near, came, weight, other, own, *sent):
    grads = jnp.concatenate([near[...], came[...]], 1)
    rows = [jnp.concatenate([w[b] for b in range(4)], 1) for w in (weight, other)]
    part = jnp.dot(grads, jnp.concatenate(rows, 0), preferred_element_type=F32)
    own[...] = part[0:T]
    for k in range(1, NX):
        sent[k - 1][...] = part[k * T : (k + 1) * T].astype(BF)


def block_sum_body(idx, own, *refs):
    *came, out = refs
    out[...] = (own[...] + sum(r[...].astype(F32) for r in came)).astype(BF)


def y_sum_body(idx, came, piece, stats, sent, total):
    z_own, y_own, c, _ = coords(idx)
    yc = y_own * NC + c
    for share in range(8):
        rows = sum(came[y * 8 + share].astype(F32) for y in range(NY))
        for k in range(3):
            plane, _, _ = place(share, yc, k)
            total[plane, k * UNIT : (k + 1) * UNIT, :] = rows[k * UNIT : (k + 1) * UNIT]
        lanes = slice(share * W, share * W + W)
        stats[:, lanes] = rows[48:56, 0:W] + rows[48:56, W : 2 * W]
    lines = jnp.concatenate([stats[0:6, b * CB : (b + 1) * CB] for b in range(4)], 0).astype(BF)
    for z in range(NZ):
        sent[z, 0:48, :] = total[z].astype(BF)
        sent[z, 48:72, :] = lines
    piece[...] = total[z_own]


def z_sum_body(scale, idx, piece, stats, came, weight_grad, param_grad):
    z_own, _, _, _ = coords(idx)
    rows = sum(came[lax.rem(z_own + k, NZ)].astype(F32) for k in range(1, NZ))
    weight_grad[...] = (piece[...] + rows[0:48]) * scale
    for b in range(4):
        lanes = slice(b * CB, (b + 1) * CB)
        param_grad[:, lanes] = (stats[0:6, lanes] + rows[48 + b * 6 : 54 + b * 6]) * scale


def program(inputs, weight_t, states, doc_ids, recur, bias, out_grad):
    idx = lax.axis_index(ALL).reshape(1)
    states, out_grad = states[0], out_grad[0]
    plane = ("y", "c", "x")
    copies, tail = pl.pallas_call(
        prepare_body,
        out_shape=[
            jax.ShapeDtypeStruct((NZ, 48, CB), BF),
            jax.ShapeDtypeStruct((2, H), F32),
        ],
        grid=(1,),
        in_specs=[
            pl.BlockSpec((48, CB), lambda i: (0, 0)),
            pl.BlockSpec((8, H), lambda i: (T // 8 - 1, 0)),
            pl.BlockSpec((1, T), lambda i: (0, 0)),
        ],
        out_specs=[
            pl.BlockSpec((NZ, 48, CB), lambda i: (0, 0, 0)),
            pl.BlockSpec((2, H), lambda i: (0, 0)),
        ],
        name="prepare",
    )(weight_t, states, doc_ids)
    column = exchange(copies, "z")

    tail = along(tail, SEQ, NZ * NY * NC, 1)
    sent = call(
        messages_body, [((T, MSG), BF)] * NX, (idx, inputs[0], states, doc_ids, out_grad, tail)
    )
    mine = [sent[0]] + [around(sent[k], "x", k) for k in range(1, NX)]
    blocks = mine + [around(m, "c", 1) for m in mine]

    (parts,) = call(choose_body, [((32, 48, CB), BF)], (idx, column))
    parts = exchange(parts, plane)

    tokens = ((8 * T, W), F32)
    *kept, ends, weight = call(
        forward_body,
        [tokens] * 7 + [((8, W), F32), ((4, 3 * W, CB), BF)],
        (idx, recur, bias, *blocks, parts),
        [
            pltpu.VMEM((8 * T, 3 * W), F32),
            pltpu.VMEM((4, 2 * T + 8, W), F32),
            pltpu.VMEM((4, 2 * T, W), F32),
        ],
    )
    one = along(ends, ("z", "y"), NZ * NY, -1)
    two = along(ends, ("z", "y"), NZ * NY, -2)
    other_weight = around(weight, "c", 1)
    near, far, sent = call(
        backward_body,
        [((4 * T, 3 * W), BF), ((4 * T, 3 * W), BF), ((32, 56, CB), BF)],
        (idx, one, two, *kept, *blocks),
        [pltpu.VMEM((4, 3 * W, CB), F32)],
    )

    far = around(far, "c", 1)
    own, *sent_x = call(
        input_grad_body,
        [((T, F), F32)] + [((T, F), BF)] * 3,
        (idx, near, far, weight, other_weight),
    )
    back = []
    for k in range(1, NX):
        back.append(around(sent_x[k - 1], "x", NX - k))
    (input_grad,) = call(block_sum_body, [((T, F), BF)], (idx, own, *back))
    came = exchange(sent, plane)
    piece, stats, sent = call(
        y_sum_body,
        [((48, CB), F32), ((8, H), F32), ((NZ, 72, CB), BF)],
        (idx, came),
        [pltpu.VMEM((NZ, 48, CB), F32)],
    )
    came = exchange(sent, "z")
    scale = 1.0 / math.sqrt(inputs.shape[0] * T * NZ * NY * NC * NX)
    weight_grad, param_grad = call(
        functools.partial(z_sum_body, scale),
        [((48, CB), F32), ((6, H), F32)],
        (idx, piece, stats, came),
    )

    return input_grad[None], weight_grad, param_grad


def solution(mesh):
    torus = Mesh(mesh.devices.reshape(NZ, NY, NC, NX), ALL)
    in_specs = (
        P("x", SEQ, None),
        P(SEQ, "x"),
        P("x", SEQ, None),
        P("x", SEQ),
        P(),
        P(),
        P("x", SEQ, None),
    )
    out_specs = (P("x", SEQ, None), P(SEQ, "x"), P())
    return jax.shard_map(
        program, mesh=torus, in_specs=in_specs, out_specs=out_specs, check_vma=False
    )
```

```python
import functools
import math

import jax
import jax.numpy as jnp
from jax import lax
from jax.experimental import pallas as pl
from jax.experimental.pallas import tpu as pltpu
from jax.sharding import Mesh
from jax.sharding import PartitionSpec as P

SEQ = ("z", "y", "c")
ALL = ("z", "y", "c", "x")
NZ, NY, NC, NX = 8, 4, 2, 4
T = 128
F = 1024
H = 1024
W = 128
UNIT = 16
CB = F // 4
FAR = 2.0
CHUNK = 32
GRANT = 20 << 20
BF = jnp.bfloat16
F32 = jnp.float32


def around(a, axis, k):
    n = lax.axis_size(axis)
    return lax.ppermute(a, axis, [(i, (i + k) % n) for i in range(n)])


def exchange(a, axes):
    return lax.all_to_all(a, axes, split_axis=0, concat_axis=0, tiled=True)


def place(share, yc, k):
    plane = lax.rem(3 * (share + 8 - ((3 * yc + k) >> 3)), 8)
    unit = 24 * plane + 3 * yc + k
    return plane, unit >> 6, unit & 7


def along(a, axis, n, k):
    return lax.ppermute(a, axis, [(i, i + k) for i in range(n) if 0 <= i + k < n])


def call(body, outs, args, scratch=(), far=(), far_outs=()):
    vmem = pl.BlockSpec(memory_space=pltpu.VMEM)
    hbm = pl.BlockSpec(memory_space=pltpu.HBM)
    smem = pl.BlockSpec(memory_space=pltpu.SMEM)
    kernel = pl.pallas_call(
        body,
        out_shape=[
            (pltpu.HBM if n in far_outs else jax.ShapeDtypeStruct)(s, d)
            for n, (s, d) in enumerate(outs)
        ],
        in_specs=[smem] + [hbm if n in far else vmem for n in range(1, len(args))],
        out_specs=[hbm if n in far_outs else vmem for n in range(len(outs))],
        scratch_shapes=list(scratch),
        compiler_params=pltpu.CompilerParams(vmem_limit_bytes=GRANT),
    )
    args = [
        pltpu.with_memory_space_constraint(a, pltpu.HBM) if n in far else a
        for n, a in enumerate(args)
    ]
    return kernel(*args)


def coords(idx):
    n = idx[0]
    return n >> 5, (n >> 3) & 3, (n >> 2) & 1, n & 3


def at(start, size, step):
    return pl.ds(pl.multiple_of(start, step), size)


def split2(v):
    high = v.astype(BF)
    return high, (v - high.astype(F32)).astype(BF)


MSG = 2 * 2 * W


def prepare_body(idx, weight, states, ids, copies, tail, block, last, number, sem):
    moves = [
        pltpu.make_async_copy(weight, block, sem.at[0]),
        pltpu.make_async_copy(states.at[pl.ds(T - 8, 8)], last, sem.at[1]),
        pltpu.make_async_copy(ids, number, sem.at[2]),
    ]
    for move in moves:
        move.start()
    for move in moves:
        move.wait()
    tail[0:1, :] = last[7:8, :]
    tail[1:2, :] = jnp.broadcast_to(number[0:1, T - 1 : T].astype(F32), (1, H))
    for z in range(NZ):
        copies[z] = block[...]


def messages_body(idx, states, ids, grads, tail, *outs):
    z, y, c, x_own = coords(idx)
    row = lax.broadcasted_iota(jnp.int32, (T, W), 0)
    lane = lax.broadcasted_iota(jnp.int32, (T, W), 1)
    number = ids[...].astype(F32)
    column = jnp.sum(jnp.where(row == lane, number, 0.0), 1, keepdims=True)
    column = jnp.broadcast_to(column, (T, W))
    before = jnp.where(row == 0, tail[1:2, 0:W], pltpu.roll(column, 1, 0))
    same = (before == column) & ((row > 0) | (z + y + c > 0))
    for k in range(NX):
        out = outs[k]
        x = lax.rem(x_own + k, NX)
        for c in range(NC):
            lanes = at(c * 512 + x * W, W, W)
            prior = jnp.where(row == 0, tail[0:1, lanes], pltpu.roll(states[:, lanes], 1, 0))
            out[:, c * W : (c + 1) * W] = jnp.where(same, prior, FAR).astype(BF)
            out[:, (2 + c) * W : (3 + c) * W] = grads[:, lanes]


def choose_body(idx, column, out):
    _, y, c, _ = coords(idx)
    yc = y * NC + c
    for share in range(8):
        for k in range(3):
            plane, _, _ = place(share, yc, k)
            rows = column[plane, k * UNIT : (k + 1) * UNIT, :]
            for to in range(NY):
                out[to * 8 + share, k * UNIT : (k + 1) * UNIT, :] = rows


def forward_body(idx, recur, bias, *refs):
    feats, mine, other, parts, *refs = refs[:8], refs[8:12], refs[12:16], *refs[16:]
    az, ac, ar, pr, rp, loc, fac, ends, weight_out, *refs = refs
    weight, pre, jac, upg, gates, tokens, sem = refs
    _, _, c, x = coords(idx)
    params = [
        pltpu.make_async_copy(recur, gates.at[0], sem.at[0]),
        pltpu.make_async_copy(bias, gates.at[1], sem.at[1]),
    ]
    for n, block in enumerate((*mine, *other)):
        params.append(pltpu.make_async_copy(block, tokens.at[n], sem.at[3 + n]))
    for move in params:
        move.start()
    share = c * 4 + x
    for yc in range(NY * NC):
        for k in range(3):
            _, gate, unit = place(share, yc, k)
            rows = at(gate * W + unit * UNIT, UNIT, UNIT)
            for b in range(NX):
                weight[b, rows, :] = parts[yc * NX + b, k * UNIT : (k + 1) * UNIT, :]
    leave = pltpu.make_async_copy(weight, weight_out, sem.at[2])
    leave.start()
    feats = jnp.concatenate([feats[k + n][...] for k in range(4) for n in (0, 4)], 0)
    rows = jnp.concatenate([weight[b] for b in range(4)], 1)
    pre[...] = lax.dot_general(feats, rows, (((1,), (1,)), ((), ())), preferred_element_type=F32)
    lanes = at(share * W, W, W)
    for move in params:
        move.wait()
    rz, rr, rc = (gates[0, g : g + 1, lanes] for g in range(3))
    bz, br, bc = (gates[1, g : g + 1, lanes] for g in range(3))
    for k in range(4):
        jac[k, 2 * T : 2 * T + 8, :] = jnp.ones((8, W), F32)
        for side in range(2):
            block = tokens.at[k + 4 * side]
            base = k * 256 + side * T
            half = lax.rem(c + side, 2) * T

            def step(i, carry, block=block, base=base, half=half, k=k):
                own = at(i * CHUNK, CHUNK, CHUNK)
                here = at(base + i * CHUNK, CHUNK, CHUNK)
                when = at(half + i * CHUNK, CHUNK, CHUNK)
                coded = block[own, at(c * W, W, W)].astype(F32)
                same = coded < 1.5
                prior = jnp.where(same, coded, 0.0)
                gz = jax.nn.sigmoid(pre[here, 0:W] + rz * prior + bz)
                gr = jax.nn.sigmoid(pre[here, W : 2 * W] + rr * prior + br)
                reset = gr * prior
                gc = jnp.tanh(pre[here, 2 * W : 3 * W] + rc * reset + bc)
                keep = 1.0 - gz
                fz = (gc - prior) * gz * keep
                fc = gz * (1.0 - gc * gc)
                side_r = prior * gr * (1.0 - gr)
                value = keep + fz * rz + fc * rc * (gr + side_r * rr)
                jac[k, when, :] = jnp.where(same, value, 0.0)
                upg[k, when, :] = block[own, at(2 * W + c * W, W, W)].astype(F32)
                az[here, :] = fz
                ac[here, :] = fc
                ar[here, :] = fc * rc * side_r
                pr[here, :] = prior
                rp[here, :] = reset
                return carry

            lax.fori_loop(0, T // CHUNK, step, 0)
    sub = lax.broadcasted_iota(jnp.int32, (8, 8, W), 1)
    for k in range(4):
        for n in range(4):
            f = jac[k, n * 64 + 1 : n * 64 + 65, :].reshape(8, 8, W)
            a = upg[k, n * 64 : n * 64 + 64, :].reshape(8, 8, W)
            for d in (1, 2, 4):
                valid = sub < 8 - d
                a = jnp.where(valid, a + f * pltpu.roll(a, 8 - d, 1), a)
                f = jnp.where(valid, f * pltpu.roll(f, 8 - d, 1), f)
            loc[k * 256 + n * 64 : k * 256 + n * 64 + 64, :] = a.reshape(64, W)
            fac[k * 256 + n * 64 : k * 256 + n * 64 + 64, :] = f.reshape(64, W)

    def chain(i, carry):
        new = []
        for k in range(4):
            a0, f0 = carry[2 * k], carry[2 * k + 1]
            here = at(k * 256 + (31 - i) * 8, 8, 8)
            f = fac[here, :]
            a = loc[here, :] + f * a0
            f = f * f0
            loc[here, :] = a
            fac[here, :] = f
            new += [jnp.broadcast_to(a[0:1], (8, W)), jnp.broadcast_to(f[0:1], (8, W))]
        return tuple(new)

    start = (jnp.zeros((8, W), F32), jnp.ones((8, W), F32)) * 4
    last = lax.fori_loop(0, 32, chain, start, unroll=4)
    for k in range(4):
        ends[k : k + 1, :] = jac[k, 0:1, :] * last[2 * k + 1][0:1]
        ends[4 + k : 5 + k, :] = jac[k, 0:1, :] * last[2 * k][0:1]
    leave.wait()


def backward_body(idx, one, two, az, ac, ar, pr, rp, loc, fac, *refs):
    feats, near, far, sent, total = refs[:8], *refs[8:]
    _, _, c, x = coords(idx)
    share = c * 4 + x
    enter = one[4:8, :] + one[0:4, :] * two[4:8, :]
    sums = (jnp.zeros((8, W), F32),) * 6
    for k in range(4):
        came = enter[k : k + 1]
        for side in range(2):
            base = k * 256 + side * T
            half = k * 256 + lax.rem(c + side, 2) * T
            grads = far if side else near

            def step(i, sums, base=base, half=half, came=came, k=k, grads=grads):
                here = at(base + i * CHUNK, CHUNK, CHUNK)
                when = at(half + i * CHUNK, CHUNK, CHUNK)
                adj = loc[when, :] + fac[when, :] * came
                gz, gc, gr = adj * az[here, :], adj * ac[here, :], adj * ar[here, :]
                prior = pr[here, :]
                rows = at(k * T + i * CHUNK, CHUNK, CHUNK)
                grads[rows, 0:W] = gz.astype(BF)
                grads[rows, W : 2 * W] = gr.astype(BF)
                grads[rows, 2 * W : 3 * W] = gc.astype(BF)
                terms = (gz, gr, gc, gz * prior, gr * prior, gc * rp[here, :])
                return tuple(s + t.reshape(CHUNK // 8, 8, W).sum(0) for s, t in zip(sums, terms))

            sums = lax.fori_loop(0, T // CHUNK, step, sums)
    feats = jnp.concatenate([b[...] for b in feats], 0)
    grads = jnp.concatenate([near[...], far[...]], 0)
    whole = lax.dot_general(grads, feats, (((0,), (0,)), ((), ())), preferred_element_type=F32)
    for b in range(4):
        total[b] = whole[:, b * CB : (b + 1) * CB]
    stats = jnp.concatenate([jnp.sum(s, 0, keepdims=True) for s in sums], 0)
    high, low = split2(jnp.concatenate([stats, jnp.zeros((2, W), F32)], 0))
    for b in range(NX):
        for yc in range(NY * NC):
            for k in range(3):
                _, gate, unit = place(share, yc, k)
                rows = at(gate * W + unit * UNIT, UNIT, UNIT)
                sent[yc, b, k * UNIT : (k + 1) * UNIT, :] = total[b, rows, :].astype(BF)
            sent[yc, b, 48:56, 0:W] = high
            sent[yc, b, 48:56, W : 2 * W] = low


def input_grad_body(idx, near, came, weight, other, own, *sent):
    grads = jnp.concatenate([near[...], came[...]], 1)
    rows = [jnp.concatenate([w[b] for b in range(4)], 1) for w in (weight, other)]
    part = jnp.dot(grads, jnp.concatenate(rows, 0), preferred_element_type=F32)
    own[...] = part[0:T]
    for k in range(1, NX):
        sent[k - 1][...] = part[k * T : (k + 1) * T].astype(BF)


def block_sum_body(idx, own, *refs):
    *came, out = refs
    out[...] = (own[...] + sum(r[...].astype(F32) for r in came)).astype(BF)


def y_sum_body(idx, came, piece, stats, sent, total):
    z_own, y_own, c, _ = coords(idx)
    yc = y_own * NC + c
    for share in range(8):
        rows = sum(came[y * 8 + share].astype(F32) for y in range(NY))
        for k in range(3):
            plane, _, _ = place(share, yc, k)
            total[plane, k * UNIT : (k + 1) * UNIT, :] = rows[k * UNIT : (k + 1) * UNIT]
        lanes = slice(share * W, share * W + W)
        stats[:, lanes] = rows[48:56, 0:W] + rows[48:56, W : 2 * W]
    lines = jnp.concatenate([stats[0:6, b * CB : (b + 1) * CB] for b in range(4)], 0).astype(BF)
    for z in range(NZ):
        sent[z, 0:48, :] = total[z].astype(BF)
        sent[z, 48:72, :] = lines
    piece[...] = total[z_own]


def z_sum_body(scale, idx, piece, stats, came, weight_grad, param_grad):
    z_own, _, _, _ = coords(idx)
    rows = sum(came[lax.rem(z_own + k, NZ)].astype(F32) for k in range(1, NZ))
    weight_grad[...] = (piece[...] + rows[0:48]) * scale
    for b in range(4):
        lanes = slice(b * CB, (b + 1) * CB)
        param_grad[:, lanes] = (stats[0:6, lanes] + rows[48 + b * 6 : 54 + b * 6]) * scale


def program(inputs, weight_t, states, doc_ids, recur, bias, out_grad):
    idx = lax.axis_index(ALL).reshape(1)
    states, out_grad = states[0], out_grad[0]
    plane = ("y", "c", "x")
    features = [inputs[0]]
    for k in range(1, NX):
        features.append(around(inputs[0], "x", k))
    features += [around(m, "c", 1) for m in features]
    copies, tail = call(
        prepare_body,
        [((NZ, 48, CB), BF), ((2, H), F32)],
        (idx, weight_t, states, doc_ids),
        [
            pltpu.VMEM((48, CB), BF),
            pltpu.VMEM((8, H), F32),
            pltpu.VMEM((1, T), jnp.int32),
            pltpu.SemaphoreType.DMA((3,)),
        ],
        far=(1, 2, 3),
    )
    column = exchange(copies, "z")

    tail = along(tail, SEQ, NZ * NY * NC, 1)
    sent = call(
        messages_body, [((T, MSG), BF)] * NX, (idx, states, doc_ids, out_grad, tail)
    )
    mine = [sent[0]]
    for k in range(1, NX):
        mine.append(around(sent[k], "x", k))
    blocks = mine + [around(m, "c", 1) for m in mine]

    (parts,) = call(choose_body, [((32, 48, CB), BF)], (idx, column))
    parts = exchange(parts, plane)

    tokens = ((8 * T, W), F32)
    *kept, ends, weight = call(
        forward_body,
        [tokens] * 7 + [((8, W), F32), ((4, 3 * W, CB), BF)],
        (idx, recur, bias, *features, *blocks, parts),
        [
            pltpu.VMEM((4, 3 * W, CB), BF),
            pltpu.VMEM((8 * T, 3 * W), F32),
            pltpu.VMEM((4, 2 * T + 8, W), F32),
            pltpu.VMEM((4, 2 * T, W), F32),
            pltpu.VMEM((2, 3, H), F32),
            pltpu.VMEM((8, T, MSG), BF),
            pltpu.SemaphoreType.DMA((11,)),
        ],
        far=(1, 2, *range(11, 19)),
        far_outs=(8,),
    )
    one = along(ends, ("z", "y"), NZ * NY, -1)
    two = along(ends, ("z", "y"), NZ * NY, -2)
    other_weight = around(weight, "c", 1)
    near, far, sent = call(
        backward_body,
        [((4 * T, 3 * W), BF), ((4 * T, 3 * W), BF), ((8, NX, 56, CB), BF)],
        (idx, one, two, *kept, *features),
        [pltpu.VMEM((4, 3 * W, CB), F32)],
    )
    sent = sent.reshape(32, 56, CB)

    far = around(far, "c", 1)
    own, *sent_x = call(
        input_grad_body,
        [((T, F), F32)] + [((T, F), BF)] * 3,
        (idx, near, far, weight, other_weight),
    )
    back = []
    for k in range(1, NX):
        back.append(around(sent_x[k - 1], "x", NX - k))
    (input_grad,) = call(block_sum_body, [((T, F), BF)], (idx, own, *back))
    came = exchange(sent, plane)
    piece, stats, sent = call(
        y_sum_body,
        [((48, CB), F32), ((8, H), F32), ((NZ, 72, CB), BF)],
        (idx, came),
        [pltpu.VMEM((NZ, 48, CB), F32)],
    )
    came = exchange(sent, "z")
    scale = 1.0 / math.sqrt(inputs.shape[0] * T * NZ * NY * NC * NX)
    weight_grad, param_grad = call(
        functools.partial(z_sum_body, scale),
        [((48, CB), F32), ((6, H), F32)],
        (idx, piece, stats, came),
    )

    return input_grad[None], weight_grad, param_grad


def solution(mesh):
    torus = Mesh(mesh.devices.reshape(NZ, NY, NC, NX), ALL)
    in_specs = (
        P("x", SEQ, None),
        P(SEQ, "x"),
        P("x", SEQ, None),
        P("x", SEQ),
        P(),
        P(),
        P("x", SEQ, None),
    )
    out_specs = (P("x", SEQ, None), P(SEQ, "x"), P())
    return jax.shard_map(
        program, mesh=torus, in_specs=in_specs, out_specs=out_specs, check_vma=False
    )
```
